32 devices in a mesh: dp: 8 (over z, core), tensor: 4 (over y, x).
Axes of the slice: x: 2, y: 2, z: 4, core: 2. Of those that a mesh axis runs over, the one named last changes fastest.
Arguments:
- inputs: bfloat16 [16, 1024, 2560], P('dp', 'tensor'), may hold values from -6 to 6
- cotangent: bfloat16 [16, 1024, 2560], P('dp', 'tensor'), may hold values from -6 to 6
- lengths: int32 [16], P('dp'), may hold values from 256 to 1024, as said below
- w_query: bfloat16 [2560, 2560], P('dp', 'tensor'), may hold values from -0.125 to 0.125
- w_key: bfloat16 [2560, 640], P('dp', 'tensor'), may hold values from -0.125 to 0.125
- w_value: bfloat16 [2560, 640], P('dp', 'tensor'), may hold values from -0.125 to 0.125
- w_out: bfloat16 [2560, 2560], P('tensor', 'dp'), may hold values from -1 to 1
- w_gate: bfloat16 [2560, 7168], P('dp', 'tensor'), may hold values from -0.125 to 0.125
- w_up: bfloat16 [2560, 7168], P('dp', 'tensor'), may hold values from -0.125 to 0.125
- w_down: bfloat16 [7168, 2560], P('tensor', 'dp'), may hold values from -0.0625 to 0.0625
- attn_gain: bfloat16 [2560], P('dp'), may hold values from 0.099609375 to 1.8984375
- mlp_gain: bfloat16 [2560], P('dp'), may hold values from 0.099609375 to 1.8984375
Outputs:
- output: bfloat16 [16, 1024, 2560], P('dp', 'tensor')
- input_grad: bfloat16 [16, 1024, 2560], P('dp', 'tensor')
- grad_query: float32 [2560, 2560], P('dp', 'tensor')
- grad_key: float32 [2560, 640], P('dp', 'tensor')
- grad_value: float32 [2560, 640], P('dp', 'tensor')
- grad_out: float32 [2560, 2560], P('tensor', 'dp')
- grad_gate: float32 [2560, 7168], P('dp', 'tensor')
- grad_up: float32 [2560, 7168], P('dp', 'tensor')
- grad_down: float32 [7168, 2560], P('tensor', 'dp')
- grad_attn_gain: float32 [2560], P('dp')
- grad_mlp_gain: float32 [2560], P('dp')
The draws below stay inside these ranges and needn't reach their ends.
Inputs may be any that keep to these rules, and one draw needn't show every extreme that they name: Positions from lengths[s] on are padding of slot s. Some slot has exactly 1024 valid positions and some exactly 256.
All inputs are finite; a program needn't handle non-finite values.
Results may differ from the reference program's by a relative error of at most 0.023.
Values may be sent and summed in bfloat16 or wider, within the bound.
A program may use at most 384 MiB of HBM per device.

```python
import math
import jax
import jax.numpy as jnp
from jax import lax

D = 2560
QH = 32
KVH = 8
HD = 80
FF = 7168
SLOT = 1024
SLOTS = 16


def draw_lengths(key, part):
    base = jax.random.fold_in(key, 7)
    first_key, second_key = jax.random.split(base)
    drawn = jax.random.randint(first_key, (SLOTS,), SLOT // 4, SLOT + 1)
    order = jax.random.permutation(second_key, SLOTS)
    drawn = drawn.at[order[0]].set(SLOT)
    drawn = drawn.at[order[1]].set(SLOT // 4)
    return drawn.astype(jnp.int32)


def level_of(stream_key, shape, cuts, low, largest):
    factor_of = 1.0
    for position, blocks in cuts:
        heights = jax.random.uniform(jax.random.fold_in(jax.random.fold_in(stream_key, 6), position), (blocks,), jnp.float32, low / len(cuts), largest / len(cuts))
        factor_of = factor_of * jnp.repeat(jnp.exp(heights), shape[position] // blocks).reshape((-1,) + (1,) * (len(shape) - 1 - position))
    return factor_of


def normal_values(stream_key, extent, scale, reach, cuts=(), held_as=jnp.bfloat16):
    array = jax.random.normal(stream_key, extent, jnp.float32) * scale
    if len(cuts) > 0:
        array = level_of(stream_key, extent, cuts, -0.22, 0.18) * array
    return jnp.clip(array, min=-reach, max=reach).astype(held_as)


def setup_inputs(seed: int = 0) -> dict:
    keys = jax.random.split(jax.random.key(seed), 13)
    inputs = normal_values(keys[0], (SLOTS, SLOT, D), 1.0, 6.0, ((0, 8), (1, 4)))
    cotangent = normal_values(keys[1], (SLOTS, SLOT, D), 1.0, 6.0, ((0, 8), (1, 4)))
    lengths = draw_lengths(jax.random.fold_in(keys[12], 71), 0)
    w_query = normal_values(keys[3], (D, QH * HD), D ** -0.5, 0.125, ((0, 8), (1, 4)))
    w_key = normal_values(keys[4], (D, KVH * HD), D ** -0.5, 0.125, ((0, 8), (1, 4)))
    w_value = normal_values(keys[5], (D, KVH * HD), D ** -0.5, 0.125, ((0, 8), (1, 4)))
    w_out = normal_values(keys[6], (QH * HD, D), (QH * HD // 64) ** -0.5, 1.0, ((0, 4), (1, 8)))
    w_gate = normal_values(keys[7], (D, FF), D ** -0.5, 0.125, ((0, 8), (1, 4)))
    w_up = normal_values(keys[8], (D, FF), D ** -0.5, 0.125, ((0, 8), (1, 4)))
    w_down = normal_values(keys[9], (FF, D), FF ** -0.5, 0.0625, ((0, 4), (1, 8)))
    attn_gain = jnp.clip(1.0 + 0.18 * jax.random.normal(keys[10], (D,), jnp.float32), 0.099609375, 1.8984375).astype(jnp.bfloat16)
    mlp_gain = jnp.clip(1.0 + 0.18 * jax.random.normal(keys[11], (D,), jnp.float32), 0.099609375, 1.8984375).astype(jnp.bfloat16)
    return {"inputs": inputs, "cotangent": cotangent, "lengths": lengths, "w_query": w_query, "w_key": w_key, "w_value": w_value, "w_out": w_out, "w_gate": w_gate, "w_up": w_up, "w_down": w_down, "attn_gain": attn_gain, "mlp_gain": mlp_gain}


EPSILON = 1e-05
ROPE_BASE = 1000000.0
EXACT = lax.Precision.HIGHEST

@jax.custom_vjp
def low(v):
    return lax.optimization_barrier(v.astype(jnp.bfloat16)).astype(jnp.float32)

@jax.custom_vjp
def low_back(v):
    return v

def low_keep(v):
    return (low(v), None)

def low_pass(kept, grad):
    return (grad,)

def back_keep(v):
    return (v, None)

def back_low(kept, grad):
    return (low(grad),)
low.defvjp(low_keep, low_pass)
low_back.defvjp(back_keep, back_low)

def rope_tables(row_count, head_width):
    halfway = head_width // 2
    frequency = jnp.exp(-math.log(ROPE_BASE) * 2.0 * jnp.arange(halfway, dtype=jnp.float32) / head_width)
    places = jnp.arange(row_count, dtype=jnp.float32)
    angles = places[:, None] * frequency[None, :]
    angles = jnp.concatenate([angles, angles], axis=1)
    return (jnp.cos(angles), jnp.sin(angles))

def rotate(values):
    halfway = values.shape[-1] // 2
    return jnp.concatenate([-values[..., halfway:], values[..., :halfway]], axis=-1)

def apply_rope(values, cosine_tab, sine_tab):
    return values * cosine_tab[:, None, :] + rotate(values) * sine_tab[:, None, :]

def norm_rows(values, gain_row):
    return values * lax.rsqrt(lax.optimization_barrier(jnp.mean(values * values, axis=-1, keepdims=True)) + EPSILON) * gain_row

def matmul(left, right):
    return jnp.dot(left, right, precision=EXACT, preferred_element_type=jnp.float32)

def slot_forward(source, length, params):
    query_w, key_w, value_w, out_w, gate_w, up_w, down_w, gain_attn, gain_mlp = params
    seq_total = source.shape[0]
    group = QH // KVH
    score_scale = 1.0 / math.sqrt(HD)
    normed = low(norm_rows(source, gain_attn))
    query_pre = low_back(matmul(normed, query_w))
    key_pre = low_back(matmul(normed, key_w))
    value_heads = low(low_back(matmul(normed, value_w))).reshape(seq_total, KVH, HD)
    cosine_tab, sine_tab = rope_tables(seq_total, HD)
    query_heads = low(apply_rope(query_pre.reshape(seq_total, QH, HD), cosine_tab, sine_tab))
    query_heads = query_heads.reshape(seq_total, KVH, group, HD)
    key_heads = low(apply_rope(key_pre.reshape(seq_total, KVH, HD), cosine_tab, sine_tab))
    block_rows = math.gcd(seq_total, 512)
    blocks = seq_total // block_rows
    query_blocks = query_heads.reshape(blocks, block_rows, KVH, group, HD)
    starts = jnp.arange(blocks, dtype=jnp.int32) * block_rows

    def attend(pieces):
        query_blk, row_start = pieces
        scores = jnp.einsum('qkgd,jkd->kgqj', query_blk, key_heads, precision=EXACT)
        scores = low_back(scores * score_scale)
        rows_at = row_start + jnp.arange(block_rows, dtype=jnp.int32)
        cols_at = jnp.arange(seq_total, dtype=jnp.int32)
        allowed = (cols_at[None, :] <= rows_at[:, None]) & (cols_at[None, :] < length)
        scores = jnp.where(allowed, scores, -1e+30)
        row_peak = lax.optimization_barrier(jnp.max(scores, axis=-1, keepdims=True))
        exponent = jnp.exp(scores - row_peak)
        prob_low = low(exponent / lax.optimization_barrier(jnp.sum(exponent, axis=-1, keepdims=True)))
        return jnp.einsum('kgqj,jkd->qkgd', prob_low, value_heads, precision=EXACT)
    attended = lax.map(jax.checkpoint(attend), (query_blocks, starts))
    attended = low(low_back(attended.reshape(seq_total, QH * HD)))
    hidden = source + low_back(matmul(attended, out_w))
    normed_mlp = low(norm_rows(hidden, gain_mlp))
    gate_pre = low_back(matmul(normed_mlp, gate_w))
    up_pre = low_back(matmul(normed_mlp, up_w))
    activated = low(gate_pre * jax.nn.sigmoid(gate_pre) * up_pre)
    return hidden + low_back(matmul(activated, down_w))

def forward(source_in, weights_in, lengths):

    def step_slot(running, slot_data):
        return (running, slot_forward(slot_data[0], slot_data[1], weights_in))
    unused, result = lax.scan(step_slot, jnp.zeros((), jnp.float32), (source_in, lengths))
    return result

def reference(inputs, cotangent, lengths, w_query, w_key, w_value, w_out, w_gate, w_up, w_down, attn_gain, mlp_gain):
    params = tuple((weight.astype(jnp.float32) for weight in (w_query, w_key, w_value, w_out, w_gate, w_up, w_down, attn_gain, mlp_gain)))
    source = inputs.astype(jnp.float32)

    def whole(source_in, weights_in):
        return forward(source_in, weights_in, lengths)
    output, pullback = jax.vjp(whole, source, params)
    valid_rows = (jnp.arange(SLOT, dtype=jnp.int32)[None, :] < lengths[:, None]).astype(jnp.float32)
    grad_source, grad_params = pullback(cotangent.astype(jnp.float32) * valid_rows[:, :, None])
    return (output.astype(jnp.bfloat16), grad_source.astype(jnp.bfloat16), grad_params[0], grad_params[1], grad_params[2], grad_params[3], grad_params[4], grad_params[5], grad_params[6], grad_params[7], grad_params[8])
```

```python
import functools
import math

import jax
import jax.numpy as jnp
from jax import lax
from jax.experimental import pallas as pl
from jax.experimental.pallas import tpu as pltpu

HD = 80
NEG = -1e30


def attn_forward_kernel(order, length, q_ref, k_ref, v_ref, o_ref, lse_ref, k_rows, m_sc, l_sc, acc_sc):
    i = pl.program_id(1)
    group, _, block = q_ref.shape

    @pl.when(i == 0)
    def _():
        k_rows[...] = k_ref[...].T

    m_sc[...] = jnp.full(m_sc.shape, NEG, jnp.float32)
    l_sc[...] = jnp.zeros(l_sc.shape, jnp.float32)
    acc_sc[...] = jnp.zeros(acc_sc.shape, jnp.float32)
    scale = 1.0 / math.sqrt(HD)
    count = jnp.minimum(i + 1, (length[0] + block - 1) // block)
    keys_at = lax.broadcasted_iota(jnp.int32, (block, block), 0)
    rows_at = lax.broadcasted_iota(jnp.int32, (block, block), 1) + i * block

    def visit(j, carry):
        at = pl.multiple_of(order[j] * block, 128)
        keys = k_rows[pl.ds(at, block), :]
        vals = v_ref[:, pl.ds(at, block)]
        keyed = keys_at + j * block
        allowed = (keyed <= rows_at) & (keyed < length[0])
        for g in range(group):
            scores = jnp.dot(keys, q_ref[g], preferred_element_type=jnp.float32) * scale
            scores = jnp.where(allowed, scores, NEG)
            peak = jnp.maximum(m_sc[g], jnp.max(scores, axis=0, keepdims=True))
            expo = jnp.exp(scores - peak)
            fade = jnp.exp(m_sc[g] - peak)
            l_sc[g] = l_sc[g] * fade + jnp.sum(expo, axis=0, keepdims=True)
            acc_sc[g] = acc_sc[g] * fade + jnp.dot(
                vals, expo.astype(jnp.bfloat16), preferred_element_type=jnp.float32
            )
            m_sc[g] = peak
        return carry

    lax.fori_loop(0, count, visit, 0)
    o_ref[...] = (acc_sc[...] / l_sc[...]).astype(o_ref.dtype)
    lse_ref[...] = m_sc[...] + jnp.log(l_sc[...])


def attn_forward(q, k, v, order, length):
    heads, _, seq = q.shape
    kv_heads = k.shape[0]
    group = heads // kv_heads
    blocks = order.shape[0]
    block = seq // blocks
    tile = lambda h, i, order, length: (h, 0, order[i])
    whole = lambda h, i, order, length: (h, 0, 0)
    return pl.pallas_call(
        attn_forward_kernel,
        out_shape=(
            jax.ShapeDtypeStruct(q.shape, jnp.bfloat16),
            jax.ShapeDtypeStruct((heads, 1, seq), jnp.float32),
        ),
        grid_spec=pltpu.PrefetchScalarGridSpec(
            num_scalar_prefetch=2,
            grid=(kv_heads, blocks),
            in_specs=[
                pl.BlockSpec((group, HD, block), tile),
                pl.BlockSpec((None, HD, seq), whole),
                pl.BlockSpec((None, HD, seq), whole),
            ],
            out_specs=[
                pl.BlockSpec((group, HD, block), tile),
                pl.BlockSpec((group, 1, block), tile),
            ],
            scratch_shapes=[
                pltpu.VMEM((seq, HD), jnp.bfloat16),
                pltpu.VMEM((group, 1, block), jnp.float32),
                pltpu.VMEM((group, 1, block), jnp.float32),
                pltpu.VMEM((group, HD, block), jnp.float32),
            ],
        ),
        compiler_params=pltpu.CompilerParams(
            dimension_semantics=("arbitrary", "arbitrary"), vmem_limit_bytes=24 << 20
        ),
        cost_estimate=pl.CostEstimate(
            flops=2 * heads * seq * seq * 256, bytes_accessed=8 * heads * HD * seq, transcendentals=heads * seq * seq // 2
        ),
        name="attn_forward",
    )(order, length, q, k, v)


def attn_back_kernel(
    order, length, q_ref, k_ref, v_ref, o_ref, lse_ref, do_ref, dq_ref, dk_ref, dv_ref, k_rows, v_rows
):
    i = pl.program_id(1)
    group, _, block = q_ref.shape
    scale = 1.0 / math.sqrt(HD)

    @pl.when(i == 0)
    def _():
        k_rows[...] = k_ref[...].T
        v_rows[...] = v_ref[...].T
        dk_ref[...] = jnp.zeros(dk_ref.shape, jnp.float32)
        dv_ref[...] = jnp.zeros(dv_ref.shape, jnp.float32)

    dq_ref[...] = jnp.zeros(dq_ref.shape, jnp.float32)
    spread = (length[0] + block - 1) // block
    count = jnp.where(i < spread, i + 1, 0)
    keys_at = lax.broadcasted_iota(jnp.int32, (block, block), 0)
    rows_at = lax.broadcasted_iota(jnp.int32, (block, block), 1) + i * block

    def visit(j, carry):
        at = pl.multiple_of(order[j] * block, 128)
        keys = k_rows[pl.ds(at, block), :]
        vals = v_rows[pl.ds(at, block), :]
        keys_t = k_ref[:, pl.ds(at, block)]
        keyed = keys_at + j * block
        allowed = (keyed <= rows_at) & (keyed < length[0])
        dk = jnp.zeros((HD, block), jnp.float32)
        dv = jnp.zeros((HD, block), jnp.float32)
        for g in range(group):
            query = q_ref[g]
            grad = do_ref[g]
            delta = jnp.sum(grad.astype(jnp.float32) * o_ref[g].astype(jnp.float32), axis=0, keepdims=True)
            scores = jnp.dot(keys, query, preferred_element_type=jnp.float32) * scale
            prob = jnp.where(allowed, jnp.exp(scores - lse_ref[g]), 0.0)
            grad_prob = jnp.dot(vals, grad, preferred_element_type=jnp.float32)
            grad_scores = (prob * (grad_prob - delta)).astype(jnp.bfloat16)
            nt = (((1,), (1,)), ((), ()))
            dv += lax.dot_general(grad, prob.astype(jnp.bfloat16), nt, preferred_element_type=jnp.float32)
            dk += lax.dot_general(query, grad_scores, nt, preferred_element_type=jnp.float32)
            dq_ref[g] += jnp.dot(keys_t, grad_scores, preferred_element_type=jnp.float32)
        dk_ref[:, pl.ds(at, block)] += dk
        dv_ref[:, pl.ds(at, block)] += dv
        return carry

    lax.fori_loop(0, count, visit, 0)
    dq_ref[...] = dq_ref[...] * scale

    @pl.when(i == pl.num_programs(1) - 1)
    def _():
        dk_ref[...] = dk_ref[...] * scale


def attn_back(q, k, v, o, lse, do, order, length):
    heads, _, seq = q.shape
    kv_heads = k.shape[0]
    group = heads // kv_heads
    blocks = order.shape[0]
    block = seq // blocks
    tile = lambda h, i, order, length: (h, 0, order[i])
    whole = lambda h, i, order, length: (h, 0, 0)
    return pl.pallas_call(
        attn_back_kernel,
        out_shape=(
            jax.ShapeDtypeStruct(q.shape, jnp.float32),
            jax.ShapeDtypeStruct(k.shape, jnp.float32),
            jax.ShapeDtypeStruct(k.shape, jnp.float32),
        ),
        grid_spec=pltpu.PrefetchScalarGridSpec(
            num_scalar_prefetch=2,
            grid=(kv_heads, blocks),
            in_specs=[
                pl.BlockSpec((group, HD, block), tile),
                pl.BlockSpec((None, HD, seq), whole),
                pl.BlockSpec((None, HD, seq), whole),
                pl.BlockSpec((group, HD, block), tile),
                pl.BlockSpec((group, 1, block), tile),
                pl.BlockSpec((group, HD, block), tile),
            ],
            out_specs=[
                pl.BlockSpec((group, HD, block), tile),
                pl.BlockSpec((None, HD, seq), whole),
                pl.BlockSpec((None, HD, seq), whole),
            ],
            scratch_shapes=[
                pltpu.VMEM((seq, HD), jnp.bfloat16),
                pltpu.VMEM((seq, HD), jnp.bfloat16),
            ],
        ),
        compiler_params=pltpu.CompilerParams(
            dimension_semantics=("arbitrary", "arbitrary"), vmem_limit_bytes=24 << 20
        ),
        cost_estimate=pl.CostEstimate(
            flops=5 * heads * seq * seq * 256, bytes_accessed=16 * heads * HD * seq, transcendentals=heads * seq * seq // 2
        ),
        name="attn_back",
    )(order, length, q, k, v, o, lse, do)


from jax.sharding import PartitionSpec as P


QH = 32
KVH = 8
EPSILON = 1e-05
ROPE_BASE = 1000000.0
F32 = jnp.float32
BF16 = jnp.bfloat16


def contract(left, right, left_dim, right_dim):
    return lax.dot_general(
        left, right, (((left_dim,), (right_dim,)), ((), ())), preferred_element_type=F32
    )


def swap(value, bit):
    return lax.ppermute(value, "tensor", [(i, i ^ bit) for i in range(4)])


def gather_rows(own):
    if lax.axis_size("tensor") != 4:
        return lax.all_gather(own, "tensor", axis=0, tiled=True)
    half = own.shape[0] // 2
    along_x = swap(own, 1)
    along_y = swap(own, 2)
    far_low = swap(along_y[:half], 1)
    far_high = swap(along_x[half:], 2)
    return jnp.concatenate([own, along_x, along_y, far_low, far_high], axis=0)


def scatter_rows(part):
    if lax.axis_size("tensor") != 4:
        return lax.psum_scatter(part, "tensor", scatter_dimension=0, tiled=True).astype(F32)
    rows = part.shape[0] // 4
    half = rows // 2
    own, by_x, by_y, far = (part[r * rows : (r + 1) * rows] for r in range(4))
    via_x = swap(far[:half], 1)
    via_y = swap(far[half:], 2)
    add = lambda a, b: (a.astype(F32) + b.astype(F32)).astype(BF16)
    by_x = jnp.concatenate([by_x[:half], add(by_x[half:], via_y)], axis=0)
    by_y = jnp.concatenate([add(by_y[:half], via_x), by_y[half:]], axis=0)
    return own.astype(F32) + swap(by_x, 1).astype(F32) + swap(by_y, 2).astype(F32)


def block_order():
    count = lax.axis_size("tensor")
    blocks = jnp.arange(count, dtype=jnp.int32)
    return blocks ^ lax.axis_index("tensor") if count == 4 else blocks


def rope_tables(order, rows):
    halfway = HD // 2
    frequency = jnp.exp(-math.log(ROPE_BASE) * 2.0 * jnp.arange(halfway, dtype=F32) / HD)
    places = (order[:, None] * rows + jnp.arange(rows, dtype=jnp.int32)).reshape(-1).astype(F32)
    angles = frequency[:, None] * places[None, :]
    angles = jnp.concatenate([angles, angles], axis=0)
    return (jnp.cos(angles), jnp.sin(angles))


def rope(values, tables):
    cosine, sine = tables
    halfway = HD // 2
    turned = jnp.concatenate([-values[:, halfway:], values[:, :halfway]], axis=1)
    return (values * cosine + turned * sine).astype(BF16)


def rope_back(grads, tables):
    cosine, sine = tables
    halfway = HD // 2
    scaled = grads * sine
    turned = jnp.concatenate([scaled[:, halfway:], -scaled[:, :halfway]], axis=1)
    return (grads * cosine + turned).astype(BF16)


def norm_rows(values, gain):
    inverse = lax.rsqrt(jnp.mean(values * values, axis=-1, keepdims=True) + EPSILON)
    return (inverse, (values * inverse * gain).astype(BF16))


def norm_back(values, inverse, gain, grad):
    scaled = grad * gain
    gain_part = jnp.sum(grad * values * inverse, axis=0)
    mean = jnp.mean(scaled * values, axis=-1, keepdims=True)
    return (inverse * scaled - values * inverse**3 * mean, gain_part)


def over_dp(value):
    return lax.all_gather(value, "dp", axis=0, tiled=True)


def sum_over_dp(value):
    return lax.psum_scatter(
        value.astype(BF16), "dp", scatter_dimension=0, tiled=True
    ).astype(F32)


def shards(
    inputs,
    cotangent,
    lengths,
    w_query,
    w_key,
    w_value,
    w_out,
    w_gate,
    w_up,
    w_down,
    attn_gain,
    mlp_gain,
):
    slots, rows, width = inputs.shape
    me = lax.axis_index("tensor")
    seq = rows * lax.axis_size("tensor")
    q_cols, k_cols = w_query.shape[1], w_key.shape[1]
    order = block_order()
    tables = rope_tables(order, rows)
    gains = over_dp(jnp.stack([attn_gain, mlp_gain], axis=1)).astype(F32)
    gain_attn, gain_mlp = gains[:, 0], gains[:, 1]

    qkv_w = over_dp(jnp.concatenate([w_query, w_key, w_value], axis=1))
    out_w = over_dp(w_out.T)
    gate_w = over_dp(w_gate)
    up_w = over_dp(w_up)
    down_w = over_dp(w_down.T)

    each = range(slots)
    source, inv_attn, normed = {}, {}, {}
    for s in each:
        source[s] = inputs[s].astype(F32)
        inv_attn[s], own = norm_rows(source[s], gain_attn)
        normed[s] = gather_rows(own)

    q, k, v, att, lse = {}, {}, {}, {}, {}
    hidden, inv_mlp, normed_mlp = {}, {}, {}
    for s in each:
        heads = contract(qkv_w, normed[s], 0, 1).reshape(-1, HD, seq)
        turned = rope(heads[: (q_cols + k_cols) // HD], tables)
        q[s], k[s] = turned[: q_cols // HD], turned[q_cols // HD :]
        v[s] = heads[(q_cols + k_cols) // HD :].astype(BF16)
        att[s], lse[s] = attn_forward(q[s], k[s], v[s], order, lengths[s : s + 1])
        part = contract(att[s].reshape(q_cols, seq), out_w, 0, 1).astype(BF16)
        hidden[s] = source[s] + scatter_rows(part)
        inv_mlp[s], own = norm_rows(hidden[s], gain_mlp)
        normed_mlp[s] = gather_rows(own)

    grad_top, grad_top_all = {}, {}
    for s in each:
        valid = me * rows + jnp.arange(rows, dtype=jnp.int32) < lengths[s]
        grad_top[s] = jnp.where(valid[:, None], cotangent[s], jnp.zeros((), BF16))
        grad_top_all[s] = gather_rows(grad_top[s])

    act, grad_gate, grad_up, outputs = {}, {}, {}, {}
    grad_mid, gain_mlp_part = {}, 0.0
    for s in each:
        gate = contract(normed_mlp[s], gate_w, 1, 0)
        up = contract(normed_mlp[s], up_w, 1, 0)
        sig = jax.nn.sigmoid(gate)
        act[s] = (gate * sig * up).astype(BF16)
        grad_act = contract(grad_top_all[s], down_w, 1, 0)
        grad_gate[s] = (grad_act * up * sig * (1.0 + gate * (1.0 - sig))).astype(BF16)
        grad_up[s] = (grad_act * gate * sig).astype(BF16)
        part = (contract(grad_gate[s], gate_w, 1, 1) + contract(grad_up[s], up_w, 1, 1)).astype(BF16)
        grad_normed = scatter_rows(part)
        back, gain_part = norm_back(hidden[s], inv_mlp[s], gain_mlp, grad_normed)
        gain_mlp_part = gain_mlp_part + gain_part
        grad_mid[s] = grad_top[s].astype(F32) + back
        part = contract(act[s], down_w, 1, 1).astype(BF16)
        outputs[s] = (hidden[s] + scatter_rows(part)).astype(BF16)

    rows_of = lambda pieces: jnp.concatenate([pieces[s] for s in each], axis=0)
    cols_of = lambda pieces: jnp.concatenate([pieces[s] for s in each], axis=1)
    down_sum = sum_over_dp(contract(rows_of(grad_top_all), rows_of(act), 0, 0))
    gate_sum = sum_over_dp(contract(rows_of(normed_mlp), rows_of(grad_gate), 0, 0))
    up_sum = sum_over_dp(contract(rows_of(normed_mlp), rows_of(grad_up), 0, 0))

    grad_mid_all, grad_qkv, input_grad = {}, {}, {}
    gain_attn_part = 0.0
    for s in each:
        grad_mid_all[s] = gather_rows(grad_mid[s].astype(BF16))
        grad_att = contract(out_w, grad_mid_all[s], 0, 1).astype(BF16).reshape(-1, HD, seq)
        dq, dk, dv = attn_back(q[s], k[s], v[s], att[s], lse[s], grad_att, order, lengths[s : s + 1])
        grad_qkv[s] = jnp.concatenate(
            [rope_back(dq, tables), rope_back(dk, tables), dv.astype(BF16)], axis=0
        ).reshape(-1, seq)
        part = contract(grad_qkv[s], qkv_w, 0, 1).astype(BF16)
        grad_normed = scatter_rows(part)
        back, gain_part = norm_back(source[s], inv_attn[s], gain_attn, grad_normed)
        gain_attn_part = gain_attn_part + gain_part
        input_grad[s] = (grad_mid[s] + back).astype(BF16)

    out_sum = sum_over_dp(
        contract(rows_of(grad_mid_all), cols_of({s: att[s].reshape(q_cols, seq) for s in each}), 0, 1)
    )
    qkv_sum = sum_over_dp(contract(rows_of(normed), cols_of(grad_qkv), 0, 1))

    gain_sums = lax.psum(jnp.stack([gain_attn_part, gain_mlp_part], axis=0), ("dp", "tensor"))
    share = width // lax.axis_size("dp")
    gain_sums = lax.dynamic_slice_in_dim(gain_sums, lax.axis_index("dp") * share, share, axis=1)
    return (
        jnp.stack([outputs[s] for s in each]),
        jnp.stack([input_grad[s] for s in each]),
        qkv_sum[:, :q_cols],
        qkv_sum[:, q_cols : q_cols + k_cols],
        qkv_sum[:, q_cols + k_cols :],
        out_sum.T,
        gate_sum,
        up_sum,
        down_sum.T,
        gain_sums[0],
        gain_sums[1],
    )


def solution(mesh):
    rows, cols, wide = P("dp", "tensor", None), P("dp", "tensor"), P("tensor", "dp")
    one = P("dp")
    return jax.shard_map(
        shards,
        mesh=mesh,
        in_specs=(rows, rows, one, cols, cols, cols, wide, cols, cols, wide, one, one),
        out_specs=(rows, rows, cols, cols, cols, wide, cols, cols, wide, one, one),
        check_vma=False,
    )
```
